32 devices in a mesh: row: 4 (over z), col: 2 (over x), dp: 4 (over y, core).
Axes of the slice: x: 2, y: 2, z: 4, core: 2. Of those that a mesh axis runs over, the one named last changes fastest.
Arguments:
- tokens: bfloat16 [1536, 6144], P('dp', 'row'), parts along dimension 0, may hold values from -120 to 120
- norm_gain: float32 [6144], P('row'), may hold values from 0.25 to 1.75
- qkv_weight: bfloat16 [6144, 3, 3072], P('row', None, 'col'), may hold values from -2.5 to 2.5
- out_weight: bfloat16 [3072, 6144], P('col', 'row'), may hold values from -0.109375 to 0.109375
Outputs:
- projected: bfloat16 [1536, 6144], P('dp', 'row'), parts along dimension 0
The draws below stay inside these ranges and needn't reach their ends.
There are 4 independent parts, one for each index of `dp`. The reference program is written for one: setup_inputs(seed, part) draws one part's arguments, and reference() takes and returns one part's arrays. A program takes and returns all parts, laid end to end along the dimension named above; an argument that names none is the same for every part. Nothing has to cross between parts.
All inputs are finite; a program needn't handle non-finite values.
Results may differ from the reference program's by a relative error of at most 0.025.
Values may be sent and summed in bfloat16 or wider, within the bound.
A program may use at most 64 MiB of HBM per device.

```python
import math
import jax
import jax.numpy as jnp
from jax import lax

D = 6144
H = 24
K = 128
SEQ = 384
N_ROW = 4


def draw_tokens(key, part):
    subkeys = jax.random.split(key, 4)
    position = jnp.arange(D, dtype=jnp.float32) / D
    texture = jnp.exp(jax.random.uniform(subkeys[0], (1, D), jnp.float32, jnp.log(0.7), jnp.log(1.4)))
    row_scale = jnp.exp(jax.random.uniform(subkeys[1], (SEQ, 1), jnp.float32, jnp.log(0.5), jnp.log(2.0)))
    offset = jnp.clip(jax.random.normal(subkeys[2], (SEQ, 1), jnp.float32), -3.0, 3.0)
    feature_ramp = 10.0 ** (position - 0.5)
    jitter = jnp.clip(jax.random.normal(subkeys[3], (SEQ, D), jnp.float32), -4.0, 4.0)
    values = row_scale * feature_ramp * (offset + jitter * texture)
    return jnp.clip(values, -120.0, 120.0).astype(jnp.bfloat16)


def draw_qkv_weight(key, part):
    subkeys = jax.random.split(key, 1)
    weights = jnp.clip(jax.random.normal(subkeys[0], (D, 3, H * K), jnp.float32), -6.0, 6.0) / math.sqrt(D)
    return jnp.clip(weights, -2.5, 2.5).astype(jnp.bfloat16)


def block_scale(own_key, dims, cuts, low, top_value):
    level = 1.0
    for axis_at, blocks in cuts:
        heights = jax.random.uniform(jax.random.fold_in(jax.random.fold_in(own_key, 6), axis_at), (blocks,), jnp.float32, low / len(cuts), top_value / len(cuts))
        level = level * jnp.repeat(jnp.exp(heights), dims[axis_at] // blocks).reshape((-1,) + (1,) * (len(dims) - 1 - axis_at))
    return level


def bell_draw(stream_key, dims, deviation, reach, shards=(), kind=jnp.bfloat16):
    level = block_scale(stream_key, dims, shards, -0.22, 0.18) if shards else 1.0
    entries = jax.random.normal(stream_key, dims, jnp.float32) * deviation * level
    return jnp.minimum(jnp.maximum(entries, -reach), reach).astype(kind)


def setup_inputs(seed: int = 0, part: int = 0) -> dict:
    key_of = jax.random.split(jax.random.key(seed), 5)
    part_splits = jax.random.split(jax.random.fold_in(key_of[4], part), 5)
    return {
        "tokens": draw_tokens(jax.random.fold_in(jax.random.fold_in(key_of[4], part), 71), part),
        "norm_gain": jnp.clip(1.0 + 0.15 * jax.random.normal(key_of[1], (D,), jnp.float32), 0.25, 1.75),
        "qkv_weight": draw_qkv_weight(jax.random.fold_in(key_of[4], 71), part),
        "out_weight": bell_draw(key_of[3], (H * K, D), (H * K) ** -0.5, 0.109375, ((0, 2), (1, 4))),
    }


EPSILON = 1e-05

def normalize(tokens, norm_gain):
    values = tokens.astype(jnp.float32)
    average = lax.optimization_barrier(jnp.mean(values, axis=1, keepdims=True))
    centered = values - average
    variance = lax.optimization_barrier(jnp.mean(centered * centered, axis=1, keepdims=True))
    return (centered * lax.rsqrt(variance + EPSILON) * norm_gain).astype(jnp.bfloat16)

def project(normed, qkv_weight):
    block_width = D // N_ROW
    flattened = qkv_weight.reshape(D, 3 * H * K)
    totals = jnp.zeros((SEQ, 3 * H * K), jnp.float32)
    for row_block in range(N_ROW):
        first_feature = row_block * block_width
        partial_value = jnp.dot(normed[:, first_feature:first_feature + block_width], flattened[first_feature:first_feature + block_width], preferred_element_type=jnp.float32)
        rounded = lax.optimization_barrier(partial_value.astype(jnp.bfloat16))
        totals = totals + rounded.astype(jnp.float32)
    return totals.astype(jnp.bfloat16).reshape(SEQ, 3, H, K)

def attend_head(operands):
    query_part, key_part, value_part = operands
    scores = jnp.dot(query_part, key_part.T, preferred_element_type=jnp.float32) * (1.0 / math.sqrt(K))
    largest = lax.optimization_barrier(jnp.max(scores, axis=1, keepdims=True))
    exponent = jnp.exp(scores - largest)
    softmax_weights = (exponent / lax.optimization_barrier(jnp.sum(exponent, axis=1, keepdims=True))).astype(jnp.bfloat16)
    return jnp.dot(softmax_weights, value_part, preferred_element_type=jnp.float32).astype(jnp.bfloat16)

def reference(tokens, norm_gain, qkv_weight, out_weight):
    normed = normalize(tokens, norm_gain)
    stacked = jnp.transpose(project(normed, qkv_weight), (1, 2, 0, 3))
    attended = lax.map(attend_head, (stacked[0], stacked[1], stacked[2]))
    attended = jnp.transpose(attended, (1, 0, 2)).reshape(SEQ, H * K)
    return jnp.dot(attended, out_weight, preferred_element_type=jnp.float32).astype(jnp.bfloat16)
```

```python
import functools
import math

import jax
import jax.numpy as jnp
from jax import lax
from jax.experimental import pallas as pl
from jax.experimental.pallas import tpu as pltpu
from jax.sharding import PartitionSpec as P

K = 128


EPSILON = 1e-05


def attend(queries, key_rows, value_rows):
    query_total = queries.shape[0]
    head_count = queries.shape[1] // K
    scaling = 1.0 / math.sqrt(K)
    split_keys = key_rows.reshape(key_rows.shape[0], head_count, K)
    split_values = value_rows.reshape(value_rows.shape[0], head_count, K)
    split_queries = queries.reshape(query_total, head_count, K)
    scores = (
        jnp.einsum("qhd,khd->hqk", split_queries, split_keys, preferred_element_type=jnp.float32)
        * scaling
    )
    largest = jnp.max(scores, axis=2, keepdims=True)
    exponent = jnp.exp(scores - largest)
    softmax_weights = (exponent / jnp.sum(exponent, axis=2, keepdims=True)).astype(jnp.bfloat16)
    mixed = jnp.einsum(
        "hqk,khd->qhd", softmax_weights, split_values, preferred_element_type=jnp.float32
    )
    result = mixed.astype(jnp.bfloat16)
    return result.reshape(query_total, head_count * K)


def shards(tokens, norm_gain, qkv_weight, out_weight):
    row_count, block_width = tokens.shape
    full_width = block_width * lax.axis_size("row")
    values = tokens.astype(jnp.float32)
    totals, squares = lax.psum(
        (jnp.sum(values, axis=1, keepdims=True), jnp.sum(values * values, axis=1, keepdims=True)),
        "row",
    )
    average = totals / full_width
    variance = squares / full_width - average * average
    centered = values - average
    normed = (centered * lax.rsqrt(variance + EPSILON) * norm_gain).astype(jnp.bfloat16)
    head_columns = qkv_weight.shape[2]
    partial_value = jnp.dot(
        normed,
        qkv_weight.reshape(block_width, 3 * head_columns),
        preferred_element_type=jnp.float32,
    )
    summed = lax.psum(partial_value.astype(jnp.bfloat16), "row").reshape(row_count, 3, head_columns)
    attended = attend(summed[:, 0], summed[:, 1], summed[:, 2])
    partial_out = jnp.dot(attended, out_weight, preferred_element_type=jnp.float32)
    return lax.psum(partial_out.astype(jnp.bfloat16), "col")


MESH = pl.DeviceIdType.MESH
WIDE = 2 * K
SKEW = 2
ROWS = 32


def sublayer_kernel(
    rows_n, cols_n, tok_hbm, gain_ref, w_hbm, wo_hbm, out_ref,
    tok, wide_w, out_w, stat_col, stats, normed, arrived, summed, attended, mine, theirs,
    tok_sem, w_sem, wo_sem, st_send, st_recv, rs_send, rs_recv, at_send, at_recv, x_send, x_recv,
):
    z = lax.axis_index("row")
    col = lax.axis_index("col")
    tokens_n, block = tok.shape
    half = w_hbm.shape[2] // 2
    pairs = half // WIDE
    chunks = 3 * pairs
    tiles = block // WIDE
    scaling = 1.0 / math.sqrt(K)

    def weight_copy(d, c):
        pair, kind = c // 3, c % 3
        first = pl.multiple_of(d * half + pair * WIDE, WIDE)
        return pltpu.make_async_copy(
            w_hbm.at[kind, :, pl.ds(first, WIDE)], wide_w.at[d, c], w_sem.at[d, c]
        )

    tok_copy = pltpu.make_async_copy(tok_hbm, tok, tok_sem)
    tok_copy.start()

    @pl.loop(0, chunks)
    def _(c):
        weight_copy(0, c).start()
        weight_copy(1, c).start()

    wo_copy = pltpu.make_async_copy(wo_hbm, out_w, wo_sem)
    wo_copy.start()

    barrier = pltpu.get_barrier_semaphore()
    for o in range(1, rows_n):
        pl.semaphore_signal(
            barrier, inc=1, device_id={"row": lax.rem(z + o, rows_n)}, device_id_type=MESH
        )
    pl.semaphore_signal(barrier, inc=1, device_id={"col": 1 - col}, device_id_type=MESH)

    tok_copy.wait()

    @pl.loop(0, tokens_n // ROWS)
    def _(i):
        at = pl.ds(pl.multiple_of(i * ROWS, ROWS), ROWS)
        x = tok[at, :].astype(jnp.float32)
        mean = jnp.sum(x, axis=1, keepdims=True) * (1.0 / block)
        away = x - mean
        square = jnp.sum(away * away, axis=1, keepdims=True)
        stat_col[0, at, :] = jnp.broadcast_to(mean, (ROWS, 128))
        stat_col[1, at, :] = jnp.broadcast_to(square, (ROWS, 128))

    stats[z, 0] = stat_col[0].T[0:8]
    stats[z, 1] = stat_col[1].T[0:8]
    pl.semaphore_wait(barrier, rows_n)

    def stat_copy(o):
        return pltpu.make_async_remote_copy(
            src_ref=stats.at[z], dst_ref=stats.at[z], send_sem=st_send.at[o],
            recv_sem=st_recv.at[z], device_id={"row": lax.rem(z + o, rows_n)},
            device_id_type=MESH,
        )

    def stat_arrival(o):
        source = lax.rem(z + o, rows_n)
        return pltpu.make_async_remote_copy(
            src_ref=stats.at[source], dst_ref=stats.at[source], send_sem=st_send.at[o],
            recv_sem=st_recv.at[source], device_id={"row": source}, device_id_type=MESH,
        )

    for o in range(1, rows_n):
        stat_copy(o).start()
    for o in range(1, rows_n):
        stat_arrival(o).wait_recv()
    mean = sum(stats[i, 0] for i in range(rows_n)) * (1.0 / rows_n)
    spread = sum(
        stats[i, 1] * (1.0 / block) + (stats[i, 0] - mean) * (stats[i, 0] - mean)
        for i in range(rows_n)
    ) * (1.0 / rows_n)
    scale = lax.rsqrt(spread + EPSILON)
    stat_col[0] = jnp.broadcast_to(mean[0:1], (128, tokens_n)).T
    stat_col[1] = jnp.broadcast_to(scale[0:1], (128, tokens_n)).T

    @pl.loop(0, tokens_n // ROWS)
    def _(i):
        at = pl.ds(pl.multiple_of(i * ROWS, ROWS), ROWS)
        x = tok[at, :].astype(jnp.float32)
        away = (x - stat_col[0, at, 0:1]) * stat_col[1, at, 0:1]
        normed[at, :] = (away * gain_ref[...]).astype(jnp.bfloat16)

    def place(d):
        return z if d == 1 else rows_n - 1 - z

    def onward(d):
        return {"row": jnp.clip(z + 1 if d == 1 else z - 1, 0, rows_n - 1)}

    def back(d):
        return {"row": jnp.clip(z - 1 if d == 1 else z + 1, 0, rows_n - 1)}

    def sum_copy(d, c):
        return pltpu.make_async_remote_copy(
            src_ref=summed.at[d, c], dst_ref=arrived.at[d, c], send_sem=rs_send.at[d, c],
            recv_sem=rs_recv.at[d, c], device_id=onward(d), device_id_type=MESH,
        )

    def attended_copy(d, p):
        return pltpu.make_async_remote_copy(
            src_ref=attended.at[d, p], dst_ref=attended.at[d, p], send_sem=at_send.at[d, p],
            recv_sem=at_recv.at[d, p], device_id=back(d), device_id_type=MESH,
        )

    def attend_pair(d, p):
        for h in range(2):
            at = slice(h * K, (h + 1) * K)
            q, k, v = (summed[d, 3 * p + kind, :, at] for kind in range(3))
            scores = lax.dot_general(
                q, k, (((1,), (1,)), ((), ())), preferred_element_type=jnp.float32
            ) * scaling
            exponent = jnp.exp(scores - jnp.max(scores, axis=1, keepdims=True))
            weights = exponent / jnp.sum(exponent, axis=1, keepdims=True)
            attended[d, p, :, at] = jnp.dot(
                weights.astype(jnp.bfloat16), v, preferred_element_type=jnp.float32
            ).astype(jnp.bfloat16)

    last_place = rows_n - 1
    slots = chunks + 2 * SKEW * last_place

    @pl.loop(0, slots)
    def _(t):
        for d in range(2):
            pos = place(d)
            c = t - SKEW * pos

            @pl.when((c >= 0) & (c < chunks))
            def _():
                weight_copy(d, c).wait()
                part = jnp.dot(normed[...], wide_w[d, c], preferred_element_type=jnp.float32)

                @pl.when(pos == 0)
                def _():
                    summed[d, c] = part.astype(jnp.bfloat16)

                @pl.when(pos > 0)
                def _():
                    sum_copy(d, c).wait_recv()
                    total = part + arrived[d, c].astype(jnp.float32)
                    summed[d, c] = total.astype(jnp.bfloat16)

                @pl.when(pos < last_place)
                def _():
                    sum_copy(d, c).start()

        for d in range(2):
            pos = place(d)
            e = t - SKEW * last_place - SKEW * (last_place - pos)
            p = e // 3

            @pl.when((e >= 0) & (e < chunks) & (e % 3 == 2))
            def _():
                @pl.when(pos == last_place)
                def _():
                    attend_pair(d, p)

                @pl.when(pos < last_place)
                def _():
                    attended_copy(d, p).wait_recv()

                @pl.when(pos > 0)
                def _():
                    attended_copy(d, p).start()

    wo_copy.wait()

    def exchange(j):
        return pltpu.make_async_remote_copy(
            src_ref=mine.at[j], dst_ref=theirs.at[j], send_sem=x_send.at[j],
            recv_sem=x_recv.at[j], device_id={"col": 1 - col}, device_id_type=MESH,
        )

    @pl.loop(0, tiles)
    def _(j):
        at = pl.ds(pl.multiple_of(j * WIDE, WIDE), WIDE)
        total = jnp.zeros((tokens_n, WIDE), jnp.float32)
        for d in range(2):
            for p in range(pairs):
                first = d * half + p * WIDE
                total = total + jnp.dot(
                    attended[d, p], out_w[first:first + WIDE, at],
                    preferred_element_type=jnp.float32,
                )
        mine[j] = total.astype(jnp.bfloat16)
        exchange(j).start()

    @pl.loop(0, tiles)
    def _(j):
        at = pl.ds(pl.multiple_of(j * WIDE, WIDE), WIDE)
        exchange(j).wait_recv()
        both = mine[j].astype(jnp.float32) + theirs[j].astype(jnp.float32)
        out_ref[:, at] = both.astype(jnp.bfloat16)

    for o in range(1, rows_n):
        stat_copy(o).wait_send()
    for d in range(2):
        pos = place(d)

        @pl.when(pos < last_place)
        def _():
            @pl.loop(0, chunks)
            def _(c):
                sum_copy(d, c).wait_send()

        @pl.when(pos > 0)
        def _():
            @pl.loop(0, pairs)
            def _(p):
                attended_copy(d, p).wait_send()

    @pl.loop(0, tiles)
    def _(j):
        exchange(j).wait_send()


def fused_shards(rows_n, cols_n, tokens, norm_gain, qkv_weight, out_weight):
    tokens_n, block = tokens.shape
    head_columns = qkv_weight.shape[2]
    pairs = head_columns // (2 * WIDE)
    chunks = 3 * pairs
    tiles = block // WIDE
    any_space = pl.BlockSpec(memory_space=pl.ANY)
    vmem = pl.BlockSpec(memory_space=pltpu.VMEM)
    dma = pltpu.SemaphoreType.DMA
    bf16, f32 = jnp.bfloat16, jnp.float32
    return pl.pallas_call(
        functools.partial(sublayer_kernel, rows_n, cols_n),
        out_shape=jax.ShapeDtypeStruct((tokens_n, block), bf16),
        in_specs=[any_space, vmem, any_space, any_space],
        out_specs=vmem,
        scratch_shapes=[
            pltpu.VMEM((tokens_n, block), bf16),
            pltpu.VMEM((2, chunks, block, WIDE), bf16),
            pltpu.VMEM((head_columns, block), bf16),
            pltpu.VMEM((2, tokens_n, 128), f32),
            pltpu.VMEM((rows_n, 2, 8, tokens_n), f32),
            pltpu.VMEM((tokens_n, block), bf16),
            pltpu.VMEM((2, chunks, tokens_n, WIDE), bf16),
            pltpu.VMEM((2, chunks, tokens_n, WIDE), bf16),
            pltpu.VMEM((2, pairs, tokens_n, WIDE), bf16),
            pltpu.VMEM((tiles, tokens_n, WIDE), bf16),
            pltpu.VMEM((tiles, tokens_n, WIDE), bf16),
            dma, dma((2, chunks)), dma,
            dma((rows_n,)), dma((rows_n,)),
            dma((2, chunks)), dma((2, chunks)),
            dma((2, pairs)), dma((2, pairs)),
            dma((tiles,)), dma((tiles,)),
        ],
        compiler_params=pltpu.CompilerParams(
            collective_id=0, has_side_effects=True, vmem_limit_bytes=60 * 1024 * 1024
        ),
    )(tokens, norm_gain.reshape(1, block), jnp.transpose(qkv_weight, (1, 0, 2)), out_weight)


def solution(mesh):
    in_specs = (P("dp", "row"), P("row"), P("row", None, "col"), P("col", "row"))
    out_specs = P("dp", "row")
    rows_n, cols_n = mesh.shape["row"], mesh.shape["col"]

    def body(tokens, norm_gain, qkv_weight, out_weight):
        tokens_n, block = tokens.shape
        fits = (
            cols_n == 2 and rows_n >= 2 and qkv_weight.shape[2] % (2 * WIDE) == 0
            and block % WIDE == 0 and tokens_n % 128 == 0
        )
        if fits:
            return fused_shards(rows_n, cols_n, tokens, norm_gain, qkv_weight, out_weight)
        return shards(tokens, norm_gain, qkv_weight, out_weight)

    return jax.shard_map(body, mesh=mesh, in_specs=in_specs, out_specs=out_specs, check_vma=False)
```

```python
import functools
import math

import jax
import jax.numpy as jnp
from jax import lax
from jax.experimental import pallas as pl
from jax.experimental.pallas import tpu as pltpu
from jax.sharding import PartitionSpec as P

K = 128


EPSILON = 1e-05


def attend(queries, key_rows, value_rows):
    query_total = queries.shape[0]
    head_count = queries.shape[1] // K
    scaling = 1.0 / math.sqrt(K)
    split_keys = key_rows.reshape(key_rows.shape[0], head_count, K)
    split_values = value_rows.reshape(value_rows.shape[0], head_count, K)
    split_queries = queries.reshape(query_total, head_count, K)
    scores = (
        jnp.einsum("qhd,khd->hqk", split_queries, split_keys, preferred_element_type=jnp.float32)
        * scaling
    )
    largest = jnp.max(scores, axis=2, keepdims=True)
    exponent = jnp.exp(scores - largest)
    softmax_weights = (exponent / jnp.sum(exponent, axis=2, keepdims=True)).astype(jnp.bfloat16)
    mixed = jnp.einsum(
        "hqk,khd->qhd", softmax_weights, split_values, preferred_element_type=jnp.float32
    )
    result = mixed.astype(jnp.bfloat16)
    return result.reshape(query_total, head_count * K)


def shards(tokens, norm_gain, qkv_weight, out_weight):
    row_count, block_width = tokens.shape
    full_width = block_width * lax.axis_size("row")
    values = tokens.astype(jnp.float32)
    totals, squares = lax.psum(
        (jnp.sum(values, axis=1, keepdims=True), jnp.sum(values * values, axis=1, keepdims=True)),
        "row",
    )
    average = totals / full_width
    variance = squares / full_width - average * average
    centered = values - average
    normed = (centered * lax.rsqrt(variance + EPSILON) * norm_gain).astype(jnp.bfloat16)
    head_columns = qkv_weight.shape[2]
    partial_value = jnp.dot(
        normed,
        qkv_weight.reshape(block_width, 3 * head_columns),
        preferred_element_type=jnp.float32,
    )
    summed = lax.psum(partial_value.astype(jnp.bfloat16), "row").reshape(row_count, 3, head_columns)
    attended = attend(summed[:, 0], summed[:, 1], summed[:, 2])
    partial_out = jnp.dot(attended, out_weight, preferred_element_type=jnp.float32)
    return lax.psum(partial_out.astype(jnp.bfloat16), "col")


MESH = pl.DeviceIdType.MESH
WIDE = 2 * K
SKEW = 2
ROWS = 32
PIECE = 128
PARTS = 2


def sublayer_kernel(
    rows_n, cols_n, tok_hbm, gain_ref, w_hbm, wo_hbm, out_ref,
    tok, wide_w, out_w, stat_col, stats, normed, arrived, summed, attended, late_w, early,
    tok_sem, w_sem, wo_sem, late_sem, st_send, st_recv, rs_send, rs_recv, at_send, at_recv,
    x_send, x_recv, lw_send, lw_recv, la_send, la_recv,
):
    z = lax.axis_index("row")
    col = lax.axis_index("col")
    tokens_n, block = tok.shape
    half = w_hbm.shape[2] // 2
    pairs = half // WIDE
    chunks = 3 * pairs
    tiles = block // WIDE
    pieces = tokens_n // PIECE
    part_rows = tokens_n // PARTS
    partner = {"col": 1 - col}
    scaling = 1.0 / math.sqrt(K)

    def weight_copy(d, c):
        pair, kind = c // 3, c % 3
        first = pl.multiple_of(d * half + pair * WIDE, WIDE)
        return pltpu.make_async_copy(
            w_hbm.at[kind, :, pl.ds(first, WIDE)], wide_w.at[d, c], w_sem.at[d, c]
        )

    tok_copy = pltpu.make_async_copy(tok_hbm, tok, tok_sem)
    tok_copy.start()

    @pl.loop(0, chunks)
    def _(c):
        weight_copy(0, c).start()
        weight_copy(1, c).start()

    wo_copy = pltpu.make_async_copy(wo_hbm, out_w, wo_sem)
    wo_copy.start()

    def late_rows(d):
        return wo_hbm.at[pl.ds(d * half + (pairs - 1) * WIDE, WIDE)]

    def late_copy(d):
        return pltpu.make_async_copy(late_rows(d), late_w.at[col, d], late_sem.at[d])

    def late_share(d):
        return pltpu.make_async_remote_copy(
            src_ref=late_rows(d), dst_ref=late_w.at[col, d], send_sem=lw_send.at[d],
            recv_sem=lw_recv.at[d], device_id=partner, device_id_type=MESH,
        )

    def late_arrival(d):
        return pltpu.make_async_remote_copy(
            src_ref=late_rows(d), dst_ref=late_w.at[1 - col, d], send_sem=lw_send.at[d],
            recv_sem=lw_recv.at[d], device_id=partner, device_id_type=MESH,
        )

    for d in range(2):
        late_copy(d).start()

    barrier = pltpu.get_barrier_semaphore()
    for o in range(1, rows_n):
        pl.semaphore_signal(
            barrier, inc=1, device_id={"row": lax.rem(z + o, rows_n)}, device_id_type=MESH
        )
    pl.semaphore_signal(barrier, inc=1, device_id=partner, device_id_type=MESH)

    tok_copy.wait()

    @pl.loop(0, tokens_n // ROWS)
    def _(i):
        at = pl.ds(pl.multiple_of(i * ROWS, ROWS), ROWS)
        x = tok[at, :].astype(jnp.float32)
        mean = jnp.sum(x, axis=1, keepdims=True) * (1.0 / block)
        away = x - mean
        square = jnp.sum(away * away, axis=1, keepdims=True)
        stat_col[0, at, :] = jnp.broadcast_to(mean, (ROWS, 128))
        stat_col[1, at, :] = jnp.broadcast_to(square, (ROWS, 128))

    stats[z, 0] = stat_col[0].T[0:8]
    stats[z, 1] = stat_col[1].T[0:8]
    pl.semaphore_wait(barrier, rows_n)

    def stat_copy(o):
        return pltpu.make_async_remote_copy(
            src_ref=stats.at[z], dst_ref=stats.at[z], send_sem=st_send.at[o],
            recv_sem=st_recv.at[z], device_id={"row": lax.rem(z + o, rows_n)},
            device_id_type=MESH,
        )

    def stat_arrival(o):
        source = lax.rem(z + o, rows_n)
        return pltpu.make_async_remote_copy(
            src_ref=stats.at[source], dst_ref=stats.at[source], send_sem=st_send.at[o],
            recv_sem=st_recv.at[source], device_id={"row": source}, device_id_type=MESH,
        )

    for o in range(1, rows_n):
        stat_copy(o).start()
    for d in range(2):
        late_share(d).start()
    for o in range(1, rows_n):
        stat_arrival(o).wait_recv()
    mean = sum(stats[i, 0] for i in range(rows_n)) * (1.0 / rows_n)
    spread = sum(
        stats[i, 1] * (1.0 / block) + (stats[i, 0] - mean) * (stats[i, 0] - mean)
        for i in range(rows_n)
    ) * (1.0 / rows_n)
    scale = lax.rsqrt(spread + EPSILON)
    stat_col[0] = jnp.broadcast_to(mean[0:1], (128, tokens_n)).T
    stat_col[1] = jnp.broadcast_to(scale[0:1], (128, tokens_n)).T

    @pl.loop(0, tokens_n // ROWS)
    def _(i):
        at = pl.ds(pl.multiple_of(i * ROWS, ROWS), ROWS)
        x = tok[at, :].astype(jnp.float32)
        away = (x - stat_col[0, at, 0:1]) * stat_col[1, at, 0:1]
        normed[at, :] = (away * gain_ref[...]).astype(jnp.bfloat16)

    def place(d):
        return z if d == 1 else rows_n - 1 - z

    def onward(d):
        return {"row": jnp.clip(z + 1 if d == 1 else z - 1, 0, rows_n - 1)}

    def back(d):
        return {"row": jnp.clip(z - 1 if d == 1 else z + 1, 0, rows_n - 1)}

    def sum_copy(d, c, i):
        at = pl.ds(i * part_rows, part_rows)
        return pltpu.make_async_remote_copy(
            src_ref=summed.at[d, c, at], dst_ref=arrived.at[d, c, at],
            send_sem=rs_send.at[d, c, i], recv_sem=rs_recv.at[d, c, i],
            device_id=onward(d), device_id_type=MESH,
        )

    def attended_copy(d, p, i):
        piece = attended.at[col, d, p, pl.ds(i * PIECE, PIECE)]
        return pltpu.make_async_remote_copy(
            src_ref=piece, dst_ref=piece, send_sem=at_send.at[d, p, i],
            recv_sem=at_recv.at[d, p, i], device_id=back(d), device_id_type=MESH,
        )

    def cross_copy(d, i, owner):
        piece = attended.at[owner, d, pairs - 1, pl.ds(i * PIECE, PIECE)]
        return pltpu.make_async_remote_copy(
            src_ref=piece, dst_ref=piece, send_sem=la_send.at[d, i],
            recv_sem=la_recv.at[d, i], device_id=partner, device_id_type=MESH,
        )

    def exchange(j, owner):
        return pltpu.make_async_remote_copy(
            src_ref=early.at[owner, j], dst_ref=early.at[owner, j], send_sem=x_send.at[j],
            recv_sem=x_recv.at[j], device_id=partner, device_id_type=MESH,
        )

    def attend_piece(d, p, i):
        rows = pl.ds(i * PIECE, PIECE)
        for h in range(2):
            at = slice(h * K, (h + 1) * K)
            q = summed[d, 3 * p, rows, at]
            k = summed[d, 3 * p + 1, :, at]
            v = summed[d, 3 * p + 2, :, at]
            scores = lax.dot_general(
                q, k, (((1,), (1,)), ((), ())), preferred_element_type=jnp.float32
            ) * scaling
            exponent = jnp.exp(scores - jnp.max(scores, axis=1, keepdims=True))
            weights = exponent / jnp.sum(exponent, axis=1, keepdims=True)
            attended[col, d, p, rows, at] = jnp.dot(
                weights.astype(jnp.bfloat16), v, preferred_element_type=jnp.float32
            ).astype(jnp.bfloat16)

    def project_early():
        @pl.loop(0, tiles)
        def _(j):
            at = pl.ds(pl.multiple_of(j * WIDE, WIDE), WIDE)
            total = jnp.zeros((tokens_n, WIDE), jnp.float32)
            for d in range(2):
                for p in range(pairs - 1):
                    first = d * half + p * WIDE
                    total = total + jnp.dot(
                        attended[col, d, p], out_w[first:first + WIDE, at],
                        preferred_element_type=jnp.float32,
                    )
            early[col, j] = total.astype(jnp.bfloat16)
            exchange(j, col).start()

    last_place = rows_n - 1
    slots = chunks + 2 * SKEW * last_place
    early_slot = chunks - 4 + SKEW * (last_place + jnp.maximum(z, last_place - z))
    wo_copy.wait()

    @pl.loop(0, slots)
    def _(t):
        for d in range(2):
            pos = place(d)
            c = t - SKEW * pos

            @pl.when((c >= 0) & (c < chunks))
            def _():
                weight_copy(d, c).wait()
                part = jnp.dot(normed[...], wide_w[d, c], preferred_element_type=jnp.float32)

                for i in range(PARTS):
                    lo = i * part_rows
                    at = pl.ds(lo, part_rows)
                    share = part[lo:lo + part_rows]

                    @pl.when(pos == 0)
                    def _():
                        summed[d, c, at] = share.astype(jnp.bfloat16)

                    @pl.when(pos > 0)
                    def _():
                        sum_copy(d, c, i).wait_recv()
                        total = share + arrived[d, c, at].astype(jnp.float32)
                        summed[d, c, at] = total.astype(jnp.bfloat16)

                    @pl.when(pos < last_place)
                    def _():
                        sum_copy(d, c, i).start()

        for d in range(2):
            pos = place(d)
            e = t - SKEW * last_place - SKEW * (last_place - pos)
            p = e // 3

            @pl.when((e >= 0) & (e < chunks) & (e % 3 == 2))
            def _():
                for i in range(pieces):
                    @pl.when(pos == last_place)
                    def _():
                        attend_piece(d, p, i)

                    @pl.when(pos < last_place)
                    def _():
                        attended_copy(d, p, i).wait_recv()

                    @pl.when(pos > 0)
                    def _():
                        attended_copy(d, p, i).start()

                    @pl.when(p == pairs - 1)
                    def _():
                        cross_copy(d, i, col).start()

        @pl.when(t == early_slot)
        def _():
            project_early()

    for d in range(2):
        late_copy(d).wait()
        late_arrival(d).wait_recv()
        for i in range(pieces):
            cross_copy(d, i, 1 - col).wait_recv()

    @pl.loop(0, tiles)
    def _(j):
        at = pl.ds(pl.multiple_of(j * WIDE, WIDE), WIDE)
        exchange(j, 1 - col).wait_recv()
        total = early[0, j].astype(jnp.float32) + early[1, j].astype(jnp.float32)
        for owner in range(2):
            for d in range(2):
                total = total + jnp.dot(
                    attended[owner, d, pairs - 1], late_w[owner, d, :, at],
                    preferred_element_type=jnp.float32,
                )
        out_ref[:, at] = total.astype(jnp.bfloat16)

    for o in range(1, rows_n):
        stat_copy(o).wait_send()
    for d in range(2):
        pos = place(d)

        @pl.when(pos < last_place)
        def _():
            @pl.loop(0, chunks)
            def _(c):
                for i in range(PARTS):
                    sum_copy(d, c, i).wait_send()

        @pl.when(pos > 0)
        def _():
            @pl.loop(0, pairs)
            def _(p):
                for i in range(pieces):
                    attended_copy(d, p, i).wait_send()

    @pl.loop(0, tiles)
    def _(j):
        exchange(j, col).wait_send()

    for d in range(2):
        late_share(d).wait_send()
        for i in range(pieces):
            cross_copy(d, i, col).wait_send()


def fused_shards(rows_n, cols_n, tokens, norm_gain, qkv_weight, out_weight):
    tokens_n, block = tokens.shape
    head_columns = qkv_weight.shape[2]
    pairs = head_columns // (2 * WIDE)
    chunks = 3 * pairs
    tiles = block // WIDE
    pieces = tokens_n // PIECE
    any_space = pl.BlockSpec(memory_space=pl.ANY)
    vmem = pl.BlockSpec(memory_space=pltpu.VMEM)
    dma = pltpu.SemaphoreType.DMA
    bf16, f32 = jnp.bfloat16, jnp.float32
    return pl.pallas_call(
        functools.partial(sublayer_kernel, rows_n, cols_n),
        out_shape=jax.ShapeDtypeStruct((tokens_n, block), bf16),
        in_specs=[any_space, vmem, any_space, any_space],
        out_specs=vmem,
        scratch_shapes=[
            pltpu.VMEM((tokens_n, block), bf16),
            pltpu.VMEM((2, chunks, block, WIDE), bf16),
            pltpu.VMEM((head_columns, block), bf16),
            pltpu.VMEM((2, tokens_n, 128), f32),
            pltpu.VMEM((rows_n, 2, 8, tokens_n), f32),
            pltpu.VMEM((tokens_n, block), bf16),
            pltpu.VMEM((2, chunks, tokens_n, WIDE), bf16),
            pltpu.VMEM((2, chunks, tokens_n, WIDE), bf16),
            pltpu.VMEM((2, 2, pairs, tokens_n, WIDE), bf16),
            pltpu.VMEM((2, 2, WIDE, block), bf16),
            pltpu.VMEM((2, tiles, tokens_n, WIDE), bf16),
            dma, dma((2, chunks)), dma, dma((2,)),
            dma((rows_n,)), dma((rows_n,)),
            dma((2, chunks, PARTS)), dma((2, chunks, PARTS)),
            dma((2, pairs, pieces)), dma((2, pairs, pieces)),
            dma((tiles,)), dma((tiles,)), dma((2,)), dma((2,)),
            dma((2, pieces)), dma((2, pieces)),
        ],
        compiler_params=pltpu.CompilerParams(
            collective_id=0, has_side_effects=True, vmem_limit_bytes=60 * 1024 * 1024
        ),
    )(tokens, norm_gain.reshape(1, block), jnp.transpose(qkv_weight, (1, 0, 2)), out_weight)


def solution(mesh):
    in_specs = (P("dp", "row"), P("row"), P("row", None, "col"), P("col", "row"))
    out_specs = P("dp", "row")
    rows_n, cols_n = mesh.shape["row"], mesh.shape["col"]

    def body(tokens, norm_gain, qkv_weight, out_weight):
        tokens_n, block = tokens.shape
        fits = (
            cols_n == 2 and rows_n >= 2 and qkv_weight.shape[2] % (2 * WIDE) == 0
            and qkv_weight.shape[2] >= 4 * WIDE
            and block % WIDE == 0 and tokens_n % 128 == 0
        )
        if fits:
            return fused_shards(rows_n, cols_n, tokens, norm_gain, qkv_weight, out_weight)
        return shards(tokens, norm_gain, qkv_weight, out_weight)

    return jax.shard_map(body, mesh=mesh, in_specs=in_specs, out_specs=out_specs, check_vma=False)
```

```python
import functools
import math

import jax
import jax.numpy as jnp
from jax import lax
from jax.experimental import pallas as pl
from jax.experimental.pallas import tpu as pltpu
from jax.sharding import PartitionSpec as P

K = 128


EPSILON = 1e-05


def attend(queries, key_rows, value_rows):
    query_total = queries.shape[0]
    head_count = queries.shape[1] // K
    scaling = 1.0 / math.sqrt(K)
    split_keys = key_rows.reshape(key_rows.shape[0], head_count, K)
    split_values = value_rows.reshape(value_rows.shape[0], head_count, K)
    split_queries = queries.reshape(query_total, head_count, K)
    scores = (
        jnp.einsum("qhd,khd->hqk", split_queries, split_keys, preferred_element_type=jnp.float32)
        * scaling
    )
    largest = jnp.max(scores, axis=2, keepdims=True)
    exponent = jnp.exp(scores - largest)
    softmax_weights = (exponent / jnp.sum(exponent, axis=2, keepdims=True)).astype(jnp.bfloat16)
    mixed = jnp.einsum(
        "hqk,khd->qhd", softmax_weights, split_values, preferred_element_type=jnp.float32
    )
    result = mixed.astype(jnp.bfloat16)
    return result.reshape(query_total, head_count * K)


def shards(tokens, norm_gain, qkv_weight, out_weight):
    row_count, block_width = tokens.shape
    full_width = block_width * lax.axis_size("row")
    values = tokens.astype(jnp.float32)
    totals, squares = lax.psum(
        (jnp.sum(values, axis=1, keepdims=True), jnp.sum(values * values, axis=1, keepdims=True)),
        "row",
    )
    average = totals / full_width
    variance = squares / full_width - average * average
    centered = values - average
    normed = (centered * lax.rsqrt(variance + EPSILON) * norm_gain).astype(jnp.bfloat16)
    head_columns = qkv_weight.shape[2]
    partial_value = jnp.dot(
        normed,
        qkv_weight.reshape(block_width, 3 * head_columns),
        preferred_element_type=jnp.float32,
    )
    summed = lax.psum(partial_value.astype(jnp.bfloat16), "row").reshape(row_count, 3, head_columns)
    attended = attend(summed[:, 0], summed[:, 1], summed[:, 2])
    partial_out = jnp.dot(attended, out_weight, preferred_element_type=jnp.float32)
    return lax.psum(partial_out.astype(jnp.bfloat16), "col")


MESH = pl.DeviceIdType.MESH
WIDE = 2 * K
SKEW = 1
ROWS = 32
PIECE = 128
PARTS = 2


def sublayer_kernel(
    rows_n, cols_n, tok_hbm, gain_ref, w_hbm, wo_hbm, out_ref,
    tok, wide_w, out_w, stat_col, stats, normed, arrived, summed, attended, late_w, early,
    tok_sem, w_sem, wo_sem, late_sem, st_send, st_recv, rs_send, rs_recv, at_send, at_recv,
    x_send, x_recv, lw_send, lw_recv, la_send, la_recv,
):
    z = lax.axis_index("row")
    col = lax.axis_index("col")
    tokens_n, block = tok.shape
    half = w_hbm.shape[2] // 2
    pairs = half // WIDE
    chunks = 3 * pairs
    tiles = block // WIDE
    pieces = tokens_n // PIECE
    part_rows = tokens_n // PARTS
    partner = {"col": 1 - col}
    scaling = 1.0 / math.sqrt(K)

    def weight_copy(d, c):
        pair, kind = c // 3, c % 3
        first = pl.multiple_of(d * half + pair * WIDE, WIDE)
        return pltpu.make_async_copy(
            w_hbm.at[kind, :, pl.ds(first, WIDE)], wide_w.at[d, c], w_sem.at[d, c]
        )

    tok_copy = pltpu.make_async_copy(tok_hbm, tok, tok_sem)
    tok_copy.start()

    @pl.loop(0, chunks)
    def _(c):
        weight_copy(0, c).start()
        weight_copy(1, c).start()

    wo_copy = pltpu.make_async_copy(wo_hbm, out_w, wo_sem)
    wo_copy.start()

    def late_rows(d):
        return wo_hbm.at[pl.ds(d * half + (pairs - 1) * WIDE, WIDE)]

    def late_copy(d):
        return pltpu.make_async_copy(late_rows(d), late_w.at[col, d], late_sem.at[d])

    def late_share(d):
        return pltpu.make_async_remote_copy(
            src_ref=late_rows(d), dst_ref=late_w.at[col, d], send_sem=lw_send.at[d],
            recv_sem=lw_recv.at[d], device_id=partner, device_id_type=MESH,
        )

    def late_arrival(d):
        return pltpu.make_async_remote_copy(
            src_ref=late_rows(d), dst_ref=late_w.at[1 - col, d], send_sem=lw_send.at[d],
            recv_sem=lw_recv.at[d], device_id=partner, device_id_type=MESH,
        )

    for d in range(2):
        late_copy(d).start()

    barrier = pltpu.get_barrier_semaphore()
    for o in range(1, rows_n):
        pl.semaphore_signal(
            barrier, inc=1, device_id={"row": lax.rem(z + o, rows_n)}, device_id_type=MESH
        )
    pl.semaphore_signal(barrier, inc=1, device_id=partner, device_id_type=MESH)

    tok_copy.wait()

    @pl.loop(0, tokens_n // ROWS)
    def _(i):
        at = pl.ds(pl.multiple_of(i * ROWS, ROWS), ROWS)
        x = tok[at, :].astype(jnp.float32)
        mean = jnp.sum(x, axis=1, keepdims=True) * (1.0 / block)
        away = x - mean
        square = jnp.sum(away * away, axis=1, keepdims=True)
        stat_col[0, at, :] = jnp.broadcast_to(mean, (ROWS, 128))
        stat_col[1, at, :] = jnp.broadcast_to(square, (ROWS, 128))

    stats[z, 0] = stat_col[0].T[0:8]
    stats[z, 1] = stat_col[1].T[0:8]
    pl.semaphore_wait(barrier, rows_n)

    def stat_copy(o):
        return pltpu.make_async_remote_copy(
            src_ref=stats.at[z], dst_ref=stats.at[z], send_sem=st_send.at[o],
            recv_sem=st_recv.at[z], device_id={"row": lax.rem(z + o, rows_n)},
            device_id_type=MESH,
        )

    def stat_arrival(o):
        source = lax.rem(z + o, rows_n)
        return pltpu.make_async_remote_copy(
            src_ref=stats.at[source], dst_ref=stats.at[source], send_sem=st_send.at[o],
            recv_sem=st_recv.at[source], device_id={"row": source}, device_id_type=MESH,
        )

    for o in range(1, rows_n):
        stat_copy(o).start()
    for d in range(2):
        late_share(d).start()
    for o in range(1, rows_n):
        stat_arrival(o).wait_recv()
    mean = sum(stats[i, 0] for i in range(rows_n)) * (1.0 / rows_n)
    spread = sum(
        stats[i, 1] * (1.0 / block) + (stats[i, 0] - mean) * (stats[i, 0] - mean)
        for i in range(rows_n)
    ) * (1.0 / rows_n)
    scale = lax.rsqrt(spread + EPSILON)
    stat_col[0] = jnp.broadcast_to(mean[0:1], (128, tokens_n)).T
    stat_col[1] = jnp.broadcast_to(scale[0:1], (128, tokens_n)).T

    @pl.loop(0, tokens_n // ROWS)
    def _(i):
        at = pl.ds(pl.multiple_of(i * ROWS, ROWS), ROWS)
        x = tok[at, :].astype(jnp.float32)
        away = (x - stat_col[0, at, 0:1]) * stat_col[1, at, 0:1]
        normed[at, :] = (away * gain_ref[...]).astype(jnp.bfloat16)

    def place(d):
        return z if d == 1 else rows_n - 1 - z

    def onward(d):
        return {"row": jnp.clip(z + 1 if d == 1 else z - 1, 0, rows_n - 1)}

    def back(d):
        return {"row": jnp.clip(z - 1 if d == 1 else z + 1, 0, rows_n - 1)}

    def sum_copy(d, c, i):
        at = pl.ds(i * part_rows, part_rows)
        return pltpu.make_async_remote_copy(
            src_ref=summed.at[d, c, at], dst_ref=arrived.at[d, c, at],
            send_sem=rs_send.at[d, c, i], recv_sem=rs_recv.at[d, c, i],
            device_id=onward(d), device_id_type=MESH,
        )

    def attended_copy(d, p, i):
        piece = attended.at[col, d, p, pl.ds(i * PIECE, PIECE)]
        return pltpu.make_async_remote_copy(
            src_ref=piece, dst_ref=piece, send_sem=at_send.at[d, p, i],
            recv_sem=at_recv.at[d, p, i], device_id=back(d), device_id_type=MESH,
        )

    def cross_copy(d, i, owner):
        piece = attended.at[owner, d, pairs - 1, pl.ds(i * PIECE, PIECE)]
        return pltpu.make_async_remote_copy(
            src_ref=piece, dst_ref=piece, send_sem=la_send.at[d, i],
            recv_sem=la_recv.at[d, i], device_id=partner, device_id_type=MESH,
        )

    def exchange(j, owner):
        return pltpu.make_async_remote_copy(
            src_ref=early.at[owner, j], dst_ref=early.at[owner, j], send_sem=x_send.at[j],
            recv_sem=x_recv.at[j], device_id=partner, device_id_type=MESH,
        )

    def attend_piece(d, p, i):
        rows = pl.ds(i * PIECE, PIECE)
        for h in range(2):
            at = slice(h * K, (h + 1) * K)
            q = summed[d, 3 * p, rows, at]
            k = summed[d, 3 * p + 1, :, at]
            v = summed[d, 3 * p + 2, :, at]
            scores = lax.dot_general(
                q, k, (((1,), (1,)), ((), ())), preferred_element_type=jnp.float32
            ) * scaling
            exponent = jnp.exp(scores - jnp.max(scores, axis=1, keepdims=True))
            weights = exponent / jnp.sum(exponent, axis=1, keepdims=True)
            attended[col, d, p, rows, at] = jnp.dot(
                weights.astype(jnp.bfloat16), v, preferred_element_type=jnp.float32
            ).astype(jnp.bfloat16)

    def project_early():
        @pl.loop(0, tiles)
        def _(j):
            at = pl.ds(pl.multiple_of(j * WIDE, WIDE), WIDE)
            total = jnp.zeros((tokens_n, WIDE), jnp.float32)
            for d in range(2):
                for p in range(pairs - 1):
                    first = d * half + p * WIDE
                    total = total + jnp.dot(
                        attended[col, d, p], out_w[first:first + WIDE, at],
                        preferred_element_type=jnp.float32,
                    )
            early[col, j] = total.astype(jnp.bfloat16)
            exchange(j, col).start()

    last_place = rows_n - 1
    slots = chunks + 2 * SKEW * last_place
    early_slot = chunks - 4 + SKEW * (last_place + jnp.maximum(z, last_place - z))

    @pl.loop(0, slots)
    def _(t):
        for d in range(2):
            pos = place(d)
            c = t - SKEW * pos

            @pl.when((c >= 0) & (c < chunks))
            def _():
                weight_copy(d, c).wait()
                part = jnp.dot(normed[...], wide_w[d, c], preferred_element_type=jnp.float32)

                for i in range(PARTS):
                    lo = i * part_rows
                    at = pl.ds(lo, part_rows)
                    share = part[lo:lo + part_rows]

                    @pl.when(pos == 0)
                    def _():
                        summed[d, c, at] = share.astype(jnp.bfloat16)

                    @pl.when(pos > 0)
                    def _():
                        sum_copy(d, c, i).wait_recv()
                        total = share + arrived[d, c, at].astype(jnp.float32)
                        summed[d, c, at] = total.astype(jnp.bfloat16)

                    @pl.when(pos < last_place)
                    def _():
                        sum_copy(d, c, i).start()

        for d in range(2):
            pos = place(d)
            e = t - SKEW * last_place - SKEW * (last_place - pos)
            p = e // 3

            @pl.when((e >= 0) & (e < chunks) & (e % 3 == 2))
            def _():
                for i in range(pieces):
                    @pl.when(pos == last_place)
                    def _():
                        attend_piece(d, p, i)

                    @pl.when(pos < last_place)
                    def _():
                        attended_copy(d, p, i).wait_recv()

                    @pl.when(pos > 0)
                    def _():
                        attended_copy(d, p, i).start()

                    @pl.when(p == pairs - 1)
                    def _():
                        cross_copy(d, i, col).start()

        @pl.when(t == early_slot)
        def _():
            wo_copy.wait()
            project_early()

    for d in range(2):
        late_copy(d).wait()
        late_arrival(d).wait_recv()
        for i in range(pieces):
            cross_copy(d, i, 1 - col).wait_recv()

    @pl.loop(0, tiles)
    def _(j):
        at = pl.ds(pl.multiple_of(j * WIDE, WIDE), WIDE)
        exchange(j, 1 - col).wait_recv()
        total = early[0, j].astype(jnp.float32) + early[1, j].astype(jnp.float32)
        for owner in range(2):
            for d in range(2):
                total = total + jnp.dot(
                    attended[owner, d, pairs - 1], late_w[owner, d, :, at],
                    preferred_element_type=jnp.float32,
                )
        out_ref[:, at] = total.astype(jnp.bfloat16)

    for o in range(1, rows_n):
        stat_copy(o).wait_send()
    for d in range(2):
        pos = place(d)

        @pl.when(pos < last_place)
        def _():
            @pl.loop(0, chunks)
            def _(c):
                for i in range(PARTS):
                    sum_copy(d, c, i).wait_send()

        @pl.when(pos > 0)
        def _():
            @pl.loop(0, pairs)
            def _(p):
                for i in range(pieces):
                    attended_copy(d, p, i).wait_send()

    @pl.loop(0, tiles)
    def _(j):
        exchange(j, col).wait_send()

    for d in range(2):
        late_share(d).wait_send()
        for i in range(pieces):
            cross_copy(d, i, col).wait_send()


def fused_shards(rows_n, cols_n, tokens, norm_gain, qkv_weight, out_weight):
    tokens_n, block = tokens.shape
    head_columns = qkv_weight.shape[2]
    pairs = head_columns // (2 * WIDE)
    chunks = 3 * pairs
    tiles = block // WIDE
    pieces = tokens_n // PIECE
    any_space = pl.BlockSpec(memory_space=pl.ANY)
    vmem = pl.BlockSpec(memory_space=pltpu.VMEM)
    dma = pltpu.SemaphoreType.DMA
    bf16, f32 = jnp.bfloat16, jnp.float32
    return pl.pallas_call(
        functools.partial(sublayer_kernel, rows_n, cols_n),
        out_shape=jax.ShapeDtypeStruct((tokens_n, block), bf16),
        in_specs=[any_space, vmem, any_space, any_space],
        out_specs=vmem,
        scratch_shapes=[
            pltpu.VMEM((tokens_n, block), bf16),
            pltpu.VMEM((2, chunks, block, WIDE), bf16),
            pltpu.VMEM((head_columns, block), bf16),
            pltpu.VMEM((2, tokens_n, 128), f32),
            pltpu.VMEM((rows_n, 2, 8, tokens_n), f32),
            pltpu.VMEM((tokens_n, block), bf16),
            pltpu.VMEM((2, chunks, tokens_n, WIDE), bf16),
            pltpu.VMEM((2, chunks, tokens_n, WIDE), bf16),
            pltpu.VMEM((2, 2, pairs, tokens_n, WIDE), bf16),
            pltpu.VMEM((2, 2, WIDE, block), bf16),
            pltpu.VMEM((2, tiles, tokens_n, WIDE), bf16),
            dma, dma((2, chunks)), dma, dma((2,)),
            dma((rows_n,)), dma((rows_n,)),
            dma((2, chunks, PARTS)), dma((2, chunks, PARTS)),
            dma((2, pairs, pieces)), dma((2, pairs, pieces)),
            dma((tiles,)), dma((tiles,)), dma((2,)), dma((2,)),
            dma((2, pieces)), dma((2, pieces)),
        ],
        compiler_params=pltpu.CompilerParams(
            collective_id=0, has_side_effects=True, vmem_limit_bytes=60 * 1024 * 1024
        ),
    )(tokens, norm_gain.reshape(1, block), jnp.transpose(qkv_weight, (1, 0, 2)), out_weight)


def solution(mesh):
    in_specs = (P("dp", "row"), P("row"), P("row", None, "col"), P("col", "row"))
    out_specs = P("dp", "row")
    rows_n, cols_n = mesh.shape["row"], mesh.shape["col"]

    def body(tokens, norm_gain, qkv_weight, out_weight):
        tokens_n, block = tokens.shape
        fits = (
            cols_n == 2 and rows_n >= 2 and qkv_weight.shape[2] % (2 * WIDE) == 0
            and qkv_weight.shape[2] >= 4 * WIDE
            and block % WIDE == 0 and tokens_n % 128 == 0
        )
        if fits:
            return fused_shards(rows_n, cols_n, tokens, norm_gain, qkv_weight, out_weight)
        return shards(tokens, norm_gain, qkv_weight, out_weight)

    return jax.shard_map(body, mesh=mesh, in_specs=in_specs, out_specs=out_specs, check_vma=False)
```

```python
import functools
import math

import jax
import jax.numpy as jnp
from jax import lax
from jax.experimental import pallas as pl
from jax.experimental.pallas import tpu as pltpu
from jax.sharding import PartitionSpec as P

K = 128


EPSILON = 1e-05


def attend(queries, key_rows, value_rows):
    query_total = queries.shape[0]
    head_count = queries.shape[1] // K
    scaling = 1.0 / math.sqrt(K)
    split_keys = key_rows.reshape(key_rows.shape[0], head_count, K)
    split_values = value_rows.reshape(value_rows.shape[0], head_count, K)
    split_queries = queries.reshape(query_total, head_count, K)
    scores = (
        jnp.einsum("qhd,khd->hqk", split_queries, split_keys, preferred_element_type=jnp.float32)
        * scaling
    )
    largest = jnp.max(scores, axis=2, keepdims=True)
    exponent = jnp.exp(scores - largest)
    softmax_weights = (exponent / jnp.sum(exponent, axis=2, keepdims=True)).astype(jnp.bfloat16)
    mixed = jnp.einsum(
        "hqk,khd->qhd", softmax_weights, split_values, preferred_element_type=jnp.float32
    )
    result = mixed.astype(jnp.bfloat16)
    return result.reshape(query_total, head_count * K)


def shards(tokens, norm_gain, qkv_weight, out_weight):
    row_count, block_width = tokens.shape
    full_width = block_width * lax.axis_size("row")
    values = tokens.astype(jnp.float32)
    totals, squares = lax.psum(
        (jnp.sum(values, axis=1, keepdims=True), jnp.sum(values * values, axis=1, keepdims=True)),
        "row",
    )
    average = totals / full_width
    variance = squares / full_width - average * average
    centered = values - average
    normed = (centered * lax.rsqrt(variance + EPSILON) * norm_gain).astype(jnp.bfloat16)
    head_columns = qkv_weight.shape[2]
    partial_value = jnp.dot(
        normed,
        qkv_weight.reshape(block_width, 3 * head_columns),
        preferred_element_type=jnp.float32,
    )
    summed = lax.psum(partial_value.astype(jnp.bfloat16), "row").reshape(row_count, 3, head_columns)
    attended = attend(summed[:, 0], summed[:, 1], summed[:, 2])
    partial_out = jnp.dot(attended, out_weight, preferred_element_type=jnp.float32)
    return lax.psum(partial_out.astype(jnp.bfloat16), "col")


MESH = pl.DeviceIdType.MESH
WIDE = 2 * K
SKEW = 1
ROWS = 32
PIECE = 128
PARTS = 2


def sublayer_kernel(
    rows_n, cols_n, tok_hbm, gain_ref, w_hbm, wo_hbm, out_ref,
    tok, wide_w, stat_col, stats, normed, arrived, summed, attended, late_w,
    tok_sem, w_sem, late_sem, st_send, st_recv, rs_send, rs_recv, at_send, at_recv,
    lw_send, lw_recv, fw_send, fw_recv, la_send, la_recv,
):
    z = lax.axis_index("row")
    col = lax.axis_index("col")
    tokens_n, block = tok.shape
    half = w_hbm.shape[2] // 2
    pairs = half // WIDE
    chunks = 3 * pairs
    tiles = block // WIDE
    pieces = tokens_n // PIECE
    part_rows = tokens_n // PARTS
    partner = {"col": 1 - col}
    scaling = 1.0 / math.sqrt(K)

    def weight_copy(d, c):
        pair, kind = c // 3, c % 3
        first = pl.multiple_of(d * half + pair * WIDE, WIDE)
        return pltpu.make_async_copy(
            w_hbm.at[kind, :, pl.ds(first, WIDE)], wide_w.at[d, c], w_sem.at[d, c]
        )

    tok_copy = pltpu.make_async_copy(tok_hbm, tok, tok_sem)
    tok_copy.start()

    @pl.loop(0, chunks)
    def _(c):
        weight_copy(0, c).start()
        weight_copy(1, c).start()

    dp = lax.axis_index("dp")
    side = dp % 2
    sibling = {"dp": dp + 1 - 2 * side}
    split = WIDE // 2

    def own_copy(d, p):
        rows = pl.ds(d * half + p * WIDE, WIDE)
        return pltpu.make_async_copy(wo_hbm.at[rows], late_w.at[col, d, p], late_sem.at[d, p])

    def share_copy(d, p, owner):
        first = pl.multiple_of(d * half + p * WIDE + side * split, split)
        at = pl.ds(pl.multiple_of(side * split, split), split)
        return pltpu.make_async_remote_copy(
            src_ref=wo_hbm.at[pl.ds(first, split)], dst_ref=late_w.at[owner, d, p, at],
            send_sem=lw_send.at[d, p], recv_sem=lw_recv.at[d, p], device_id=partner,
            device_id_type=MESH,
        )

    def hand_copy(d, p, which):
        piece = late_w.at[1 - col, d, p, pl.ds(pl.multiple_of(which * split, split), split)]
        return pltpu.make_async_remote_copy(
            src_ref=piece, dst_ref=piece, send_sem=fw_send.at[d, p],
            recv_sem=fw_recv.at[d, p], device_id=sibling, device_id_type=MESH,
        )

    blocks = [(d, p) for p in range(pairs) for d in range(2)]
    for d, p in blocks:
        own_copy(d, p).start()

    barrier = pltpu.get_barrier_semaphore()
    for o in range(1, rows_n):
        pl.semaphore_signal(
            barrier, inc=1, device_id={"row": lax.rem(z + o, rows_n)}, device_id_type=MESH
        )
    pl.semaphore_signal(barrier, inc=1, device_id=partner, device_id_type=MESH)
    pl.semaphore_signal(barrier, inc=1, device_id=sibling, device_id_type=MESH)

    tok_copy.wait()

    @pl.loop(0, tokens_n // ROWS)
    def _(i):
        at = pl.ds(pl.multiple_of(i * ROWS, ROWS), ROWS)
        x = tok[at, :].astype(jnp.float32)
        mean = jnp.sum(x, axis=1, keepdims=True) * (1.0 / block)
        away = x - mean
        square = jnp.sum(away * away, axis=1, keepdims=True)
        stat_col[0, at, :] = jnp.broadcast_to(mean, (ROWS, 128))
        stat_col[1, at, :] = jnp.broadcast_to(square, (ROWS, 128))

    stats[z, 0] = stat_col[0].T[0:8]
    stats[z, 1] = stat_col[1].T[0:8]
    pl.semaphore_wait(barrier, rows_n + 1)

    def stat_copy(o):
        return pltpu.make_async_remote_copy(
            src_ref=stats.at[z], dst_ref=stats.at[z], send_sem=st_send.at[o],
            recv_sem=st_recv.at[z], device_id={"row": lax.rem(z + o, rows_n)},
            device_id_type=MESH,
        )

    def stat_arrival(o):
        source = lax.rem(z + o, rows_n)
        return pltpu.make_async_remote_copy(
            src_ref=stats.at[source], dst_ref=stats.at[source], send_sem=st_send.at[o],
            recv_sem=st_recv.at[source], device_id={"row": source}, device_id_type=MESH,
        )

    for o in range(1, rows_n):
        stat_copy(o).start()
    for d, p in blocks:
        share_copy(d, p, col).start()
    for o in range(1, rows_n):
        stat_arrival(o).wait_recv()
    mean = sum(stats[i, 0] for i in range(rows_n)) * (1.0 / rows_n)
    spread = sum(
        stats[i, 1] * (1.0 / block) + (stats[i, 0] - mean) * (stats[i, 0] - mean)
        for i in range(rows_n)
    ) * (1.0 / rows_n)
    scale = lax.rsqrt(spread + EPSILON)
    stat_col[0] = jnp.broadcast_to(mean[0:1], (128, tokens_n)).T
    stat_col[1] = jnp.broadcast_to(scale[0:1], (128, tokens_n)).T

    @pl.loop(0, tokens_n // ROWS)
    def _(i):
        at = pl.ds(pl.multiple_of(i * ROWS, ROWS), ROWS)
        x = tok[at, :].astype(jnp.float32)
        away = (x - stat_col[0, at, 0:1]) * stat_col[1, at, 0:1]
        normed[at, :] = (away * gain_ref[...]).astype(jnp.bfloat16)

    def place(d):
        return z if d == 1 else rows_n - 1 - z

    def onward(d):
        return {"row": jnp.clip(z + 1 if d == 1 else z - 1, 0, rows_n - 1)}

    def back(d):
        return {"row": jnp.clip(z - 1 if d == 1 else z + 1, 0, rows_n - 1)}

    def sum_copy(d, c, i):
        at = pl.ds(i * part_rows, part_rows)
        return pltpu.make_async_remote_copy(
            src_ref=summed.at[d, c, at], dst_ref=arrived.at[d, c, at],
            send_sem=rs_send.at[d, c, i], recv_sem=rs_recv.at[d, c, i],
            device_id=onward(d), device_id_type=MESH,
        )

    def attended_copy(d, p, i):
        piece = attended.at[col, d, p, pl.ds(i * PIECE, PIECE)]
        return pltpu.make_async_remote_copy(
            src_ref=piece, dst_ref=piece, send_sem=at_send.at[d, p, i],
            recv_sem=at_recv.at[d, p, i], device_id=back(d), device_id_type=MESH,
        )

    def cross_copy(d, p, i, owner):
        piece = attended.at[owner, d, p, pl.ds(i * PIECE, PIECE)]
        return pltpu.make_async_remote_copy(
            src_ref=piece, dst_ref=piece, send_sem=la_send.at[d, p, i],
            recv_sem=la_recv.at[d, p, i], device_id=partner, device_id_type=MESH,
        )

    def attend_piece(d, p, i):
        rows = pl.ds(i * PIECE, PIECE)
        for h in range(2):
            at = slice(h * K, (h + 1) * K)
            q = summed[d, 3 * p, rows, at]
            k = summed[d, 3 * p + 1, :, at]
            v = summed[d, 3 * p + 2, :, at]
            scores = lax.dot_general(
                q, k, (((1,), (1,)), ((), ())), preferred_element_type=jnp.float32
            ) * scaling
            exponent = jnp.exp(scores - jnp.max(scores, axis=1, keepdims=True))
            weights = exponent / jnp.sum(exponent, axis=1, keepdims=True)
            attended[col, d, p, rows, at] = jnp.dot(
                weights.astype(jnp.bfloat16), v, preferred_element_type=jnp.float32
            ).astype(jnp.bfloat16)

    last_place = rows_n - 1
    slots = chunks + 2 * SKEW * last_place
    hand_slots = [min(4 + 2 * b, slots - 1) for b in range(len(blocks))]

    @pl.loop(0, slots)
    def _(t):
        for d in range(2):
            pos = place(d)
            c = t - SKEW * pos

            @pl.when((c >= 0) & (c < chunks))
            def _():
                weight_copy(d, c).wait()
                part = jnp.dot(normed[...], wide_w[d, c], preferred_element_type=jnp.float32)

                for i in range(PARTS):
                    lo = i * part_rows
                    at = pl.ds(lo, part_rows)
                    share = part[lo:lo + part_rows]

                    @pl.when(pos == 0)
                    def _():
                        summed[d, c, at] = share.astype(jnp.bfloat16)

                    @pl.when(pos > 0)
                    def _():
                        sum_copy(d, c, i).wait_recv()
                        total = share + arrived[d, c, at].astype(jnp.float32)
                        summed[d, c, at] = total.astype(jnp.bfloat16)

                    @pl.when(pos < last_place)
                    def _():
                        sum_copy(d, c, i).start()

        for d in range(2):
            pos = place(d)
            e = t - SKEW * last_place - SKEW * (last_place - pos)
            p = e // 3

            @pl.when((e >= 0) & (e < chunks) & (e % 3 == 2))
            def _():
                for i in range(pieces):
                    @pl.when(pos == last_place)
                    def _():
                        attend_piece(d, p, i)

                    @pl.when(pos < last_place)
                    def _():
                        attended_copy(d, p, i).wait_recv()

                    @pl.when(pos > 0)
                    def _():
                        attended_copy(d, p, i).start()

                    cross_copy(d, p, i, col).start()

        for (d, p), slot in zip(blocks, hand_slots):
            @pl.when(t == slot)
            def _():
                share_copy(d, p, 1 - col).wait_recv()
                hand_copy(d, p, side).start()

    for d, p in blocks:
        own_copy(d, p).wait()
        hand_copy(d, p, 1 - side).wait_recv()
        for i in range(pieces):
            cross_copy(d, p, i, 1 - col).wait_recv()

    @pl.loop(0, tiles)
    def _(j):
        at = pl.ds(pl.multiple_of(j * WIDE, WIDE), WIDE)
        total = jnp.zeros((tokens_n, WIDE), jnp.float32)
        for owner in range(2):
            for d, p in blocks:
                total = total + jnp.dot(
                    attended[owner, d, p], late_w[owner, d, p, :, at],
                    preferred_element_type=jnp.float32,
                )
        out_ref[:, at] = total.astype(jnp.bfloat16)

    for o in range(1, rows_n):
        stat_copy(o).wait_send()
    for d in range(2):
        pos = place(d)

        @pl.when(pos < last_place)
        def _():
            @pl.loop(0, chunks)
            def _(c):
                for i in range(PARTS):
                    sum_copy(d, c, i).wait_send()

        @pl.when(pos > 0)
        def _():
            @pl.loop(0, pairs)
            def _(p):
                for i in range(pieces):
                    attended_copy(d, p, i).wait_send()

    for d, p in blocks:
        share_copy(d, p, col).wait_send()
        hand_copy(d, p, side).wait_send()
        for i in range(pieces):
            cross_copy(d, p, i, col).wait_send()


def fused_shards(rows_n, cols_n, tokens, norm_gain, qkv_weight, out_weight):
    tokens_n, block = tokens.shape
    head_columns = qkv_weight.shape[2]
    pairs = head_columns // (2 * WIDE)
    chunks = 3 * pairs
    pieces = tokens_n // PIECE
    any_space = pl.BlockSpec(memory_space=pl.ANY)
    vmem = pl.BlockSpec(memory_space=pltpu.VMEM)
    dma = pltpu.SemaphoreType.DMA
    bf16, f32 = jnp.bfloat16, jnp.float32
    return pl.pallas_call(
        functools.partial(sublayer_kernel, rows_n, cols_n),
        out_shape=jax.ShapeDtypeStruct((tokens_n, block), bf16),
        in_specs=[any_space, vmem, any_space, any_space],
        out_specs=vmem,
        scratch_shapes=[
            pltpu.VMEM((tokens_n, block), bf16),
            pltpu.VMEM((2, chunks, block, WIDE), bf16),
            pltpu.VMEM((2, tokens_n, 128), f32),
            pltpu.VMEM((rows_n, 2, 8, tokens_n), f32),
            pltpu.VMEM((tokens_n, block), bf16),
            pltpu.VMEM((2, chunks, tokens_n, WIDE), bf16),
            pltpu.VMEM((2, chunks, tokens_n, WIDE), bf16),
            pltpu.VMEM((2, 2, pairs, tokens_n, WIDE), bf16),
            pltpu.VMEM((2, 2, pairs, WIDE, block), bf16),
            dma, dma((2, chunks)), dma((2, pairs)),
            dma((rows_n,)), dma((rows_n,)),
            dma((2, chunks, PARTS)), dma((2, chunks, PARTS)),
            dma((2, pairs, pieces)), dma((2, pairs, pieces)),
            dma((2, pairs)), dma((2, pairs)), dma((2, pairs)), dma((2, pairs)),
            dma((2, pairs, pieces)), dma((2, pairs, pieces)),
        ],
        compiler_params=pltpu.CompilerParams(
            collective_id=0, has_side_effects=True, vmem_limit_bytes=60 * 1024 * 1024
        ),
    )(tokens, norm_gain.reshape(1, block), jnp.transpose(qkv_weight, (1, 0, 2)), out_weight)


def solution(mesh):
    in_specs = (P("dp", "row"), P("row"), P("row", None, "col"), P("col", "row"))
    out_specs = P("dp", "row")
    rows_n, cols_n = mesh.shape["row"], mesh.shape["col"]

    def body(tokens, norm_gain, qkv_weight, out_weight):
        tokens_n, block = tokens.shape
        fits = (
            cols_n == 2 and mesh.shape["dp"] % 2 == 0 and rows_n >= 2 and qkv_weight.shape[2] % (2 * WIDE) == 0
            and qkv_weight.shape[2] >= 4 * WIDE
            and block % WIDE == 0 and tokens_n % 128 == 0
        )
        if fits:
            return fused_shards(rows_n, cols_n, tokens, norm_gain, qkv_weight, out_weight)
        return shards(tokens, norm_gain, qkv_weight, out_weight)

    return jax.shard_map(body, mesh=mesh, in_specs=in_specs, out_specs=out_specs, check_vma=False)
```
